32 devices in a mesh: slab: 16 (over z, y, core), sub: 2 (over x).
Axes of the slice: x: 2, y: 2, z: 4, core: 2. Of those that a mesh axis runs over, the one named last changes fastest.
Arguments:
- modes: float32 [16, 2, 3, 16, 2048], P('slab', 'sub'), may hold values from -1.8 to 1.8
- connect: int32 [16, 2, 27, 256], P('slab', 'sub'), may hold values from 0 to 2559, as said below
- ghosts: int32 [16, 2, 512], P('slab', 'sub'), may hold values from 0 to 4607, as said below
- inv_jacobian: float32 [16, 2, 3, 3, 27, 256], P('slab', 'sub'), may hold values from -1.05 to 3, as said below
- young: float32 [16, 2, 256], P('slab', 'sub'), may hold values from 0.5 to 2
- density: float32 [16, 2, 256], P('slab', 'sub'), may hold values from 0.5 to 2
- ffd_cell: int32 [16, 2, 3, 2048], P('slab', 'sub'), may hold values from 0 to 4
- ffd_param: float32 [16, 2, 3, 2048], P('slab', 'sub'), may hold values from 0 to 1
- eigen: float32 [16], replicated, may hold values from 4 to 16
Outputs:
- freq_grad: float32 [3, 16, 4096], P(None, 'sub', 'slab')
The draws below stay inside these ranges and needn't reach their ends.
Inputs may be any that keep to these rules, and one draw needn't show every extreme that they name: `connect`: slots 0 to 2047 are owned, the rest ghost slots; the first 128 elements of every device name owned slots only. `ghosts`: entry (3 a + b) * 512 + n names owned node n < 512 of device ((s + a - 1) mod 16, r + b - 1), never (a, b) = (1, 1), and r + b - 1 always lies in 0 to 1. `inv_jacobian`: every 3 x 3 block has a positive determinant.
All inputs are finite; a program needn't handle non-finite values.
Results may differ from the reference program's by a relative error of at most 0.0003.
Values sent between devices are 32-bit elements; how exact they have to be, the bound alone decides.
No kernel may reach another device: no remote copies, remote signals or barrier semaphores. Data moves between devices by JAX's collectives and lax.ppermute only.
A program may use at most 64 MiB of HBM per device.

```python
import math
import jax
import jax.numpy as jnp
import numpy as np
from jax import lax

MODES = 16
CTRL = 16
ELNODES = 27
QPTS = 27
NOWN = 2048
NCP = 4096
CELLS = 5
IFACE = 512
GHOST = 512
SLOTS = 2560
ELEMS = 256
INNER = 128
N_SLAB = 16
N_SUB = 2


def draw_connect(key, part):
    base = jax.random.fold_in(key, 11)
    first, second, third = jax.random.split(base, 3)
    dims = (N_SLAB, N_SUB, ELNODES, ELEMS)
    owned = jax.random.randint(first, dims, 0, NOWN)
    ghost_slot = NOWN + jax.random.randint(second, dims, 0, GHOST)
    pick = jax.random.randint(third, dims, 0, 2)
    inner = (jnp.arange(ELEMS) < INNER)[None, None, None, :]
    return jnp.where(inner | (pick == 0), owned, ghost_slot).astype(jnp.int32)


def draw_ghosts(key, part):
    base = jax.random.fold_in(key, 23)
    first, second = jax.random.split(base, 2)
    dims = (N_SLAB, N_SUB, GHOST)
    which = jax.random.randint(first, dims, 0, 8)
    block_id = which + (which >= 4).astype(jnp.int32)
    slab_off = block_id // 3
    sub_off = block_id % 3
    sub_pos = jnp.arange(N_SUB)[None, :, None]
    sub_off = jnp.where((sub_pos == 0) & (sub_off == 0), 2, sub_off)
    sub_off = jnp.where((sub_pos == N_SUB - 1) & (sub_off == 2), 0, sub_off)
    node_at = jax.random.randint(second, dims, 0, IFACE)
    return ((slab_off * 3 + sub_off) * IFACE + node_at).astype(jnp.int32)


def draw_inv_jacobian(key, part):
    base = jax.random.fold_in(key, 51)
    first, second = jax.random.split(base, 2)
    dims = (N_SLAB, N_SUB, 1, 1, QPTS, ELEMS)
    scales = jnp.exp(jax.random.uniform(first, dims, jnp.float32, jnp.log(0.5), jnp.log(2.0)))
    spread = 0.3
    offdiag = jax.random.uniform(second, (N_SLAB, N_SUB, 3, 3, QPTS, ELEMS), jnp.float32, -spread, spread)
    identity = (jnp.arange(3)[:, None] == jnp.arange(3)[None, :]).astype(jnp.float32)[None, None, :, :, None, None]
    return (scales * (identity + offdiag * (1.0 - identity))).astype(jnp.float32)


def plant(result, own_key, low, largest):
    longest = result.shape.index(max(result.shape))
    spots = []
    for shift in (0, 1):
        where = [jax.random.randint(jax.random.fold_in(own_key, axis), (), 0, length) for axis, length in enumerate(result.shape)]
        where[longest] = (where[longest] + shift) % result.shape[longest]
        spots.append(tuple(where))
    return result.at[spots[0]].set(low).at[spots[1]].set(largest)


def levels(rng, shape, cuts, smallest, high):
    level = 1.0
    for axis_at, blocks in cuts:
        draws = jax.random.uniform(jax.random.fold_in(jax.random.fold_in(rng, 6), axis_at), (blocks,), jnp.float32, smallest / len(cuts), high / len(cuts))
        level = level * jnp.repeat(jnp.exp(draws), shape[axis_at] // blocks).reshape((-1,) + (1,) * (len(shape) - 1 - axis_at))
    return level


def noise(own_key, shape, deviation, limit, cuts=(), kind=jnp.bfloat16):
    level = levels(own_key, shape, cuts, -0.22, 0.18) if cuts else 1.0
    entries = jax.random.normal(own_key, shape, jnp.float32) * deviation * level
    return jnp.minimum(jnp.maximum(entries, -limit), limit).astype(kind)


def setup_inputs(seed: int = 0) -> dict:
    key_list = jax.random.split(jax.random.key(seed), 10)
    return {
        "modes": noise(key_list[0], (N_SLAB, N_SUB, 3, MODES, NOWN), 0.3, 1.8, ((0, 16), (1, 2)), jnp.float32),
        "connect": draw_connect(jax.random.fold_in(key_list[9], 71), 0),
        "ghosts": draw_ghosts(jax.random.fold_in(key_list[9], 71), 0),
        "inv_jacobian": draw_inv_jacobian(jax.random.fold_in(key_list[9], 71), 0),
        "young": jnp.clip(jnp.exp(math.log(2.0) - 1.3862944 * jax.random.uniform(key_list[4], (N_SLAB, N_SUB, ELEMS), jnp.float32) ** levels(key_list[4], (N_SLAB, N_SUB, ELEMS), ((0, 16), (1, 2)), -0.2, 0.2)), 0.5, 2.0),
        "density": jnp.clip(jnp.exp(math.log(2.0) - 1.3862944 * jax.random.uniform(key_list[5], (N_SLAB, N_SUB, ELEMS), jnp.float32) ** levels(key_list[5], (N_SLAB, N_SUB, ELEMS), ((0, 16), (1, 2)), -0.2, 0.2)), 0.5, 2.0),
        "ffd_cell": plant(jax.random.randint(key_list[6], (N_SLAB, N_SUB, 3, NOWN), 0, CELLS), jax.random.fold_in(key_list[6], 1), 0, CELLS - 1).astype(jnp.int32),
        "ffd_param": jnp.clip(1.0 * jax.random.uniform(key_list[7], (N_SLAB, N_SUB, 3, NOWN), jnp.float32) ** levels(key_list[7], (N_SLAB, N_SUB, 3, NOWN), ((0, 16), (1, 2)), -0.2, 0.2), 0.0, 1.0),
        "eigen": jnp.clip(jnp.exp(jax.random.uniform(key_list[8], (MODES,), jnp.float32, math.log(4.0), math.log(16.0))), 4.0, 16.0),
    }


def triple_product(first, second, third):
    table = first[:, None, None, :, None, None] * second[None, :, None, None, :, None] * third[None, None, :, None, None, :]
    return table.reshape(27, 27)

def lagrange_tables():
    points = np.array([-math.sqrt(0.6), 0.0, math.sqrt(0.6)])
    gauss_weights = np.array([5.0 / 9.0, 8.0 / 9.0, 5.0 / 9.0])
    basis = np.stack([points * (points - 1.0) / 2.0, 1.0 - points * points, points * (points + 1.0) / 2.0], axis=1)
    slopes = np.stack([points - 0.5, -2.0 * points, points + 0.5], axis=1)
    shape_fn = triple_product(basis, basis, basis)
    grad_x = triple_product(slopes, basis, basis)
    grad_y = triple_product(basis, slopes, basis)
    grad_z = triple_product(basis, basis, slopes)
    gradients = np.concatenate([grad_x, grad_y, grad_z], axis=0)
    quad_weights = (gauss_weights[:, None, None] * gauss_weights[None, :, None] * gauss_weights[None, None, :]).reshape(27)
    return (shape_fn, gradients, quad_weights)

def element_block(values, inv_jac, young_e, density_e, eigen):
    shape_np, grads_np, weights_np = lagrange_tables()
    shape_fn = jnp.asarray(shape_np, jnp.float32)
    gradients = jnp.asarray(grads_np, jnp.float32)
    quad_weights = jnp.asarray(weights_np, jnp.float32)
    highest = lax.Precision.HIGHEST
    modes_n = eigen.shape[0]
    elems = values.shape[2]
    ref_grad = jnp.einsum('xa,zae->xze', gradients, values, precision=highest).reshape(3, 27, 3, modes_n, elems)
    at_points = jnp.einsum('qa,zae->qze', shape_fn, values, precision=highest).reshape(27, 3, modes_n, elems)
    jac = [[inv_jac[ref_dir, comp_b][:, None, :] for comp_b in range(3)] for ref_dir in range(3)]
    disp = [[ref_grad[0][:, comp_a] * jac[0][comp_b] + ref_grad[1][:, comp_a] * jac[1][comp_b] + ref_grad[2][:, comp_a] * jac[2][comp_b] for comp_b in range(3)] for comp_a in range(3)]
    trace_h = disp[0][0] + disp[1][1] + disp[2][2]
    lame = 0.3 / 0.52 * young_e[None, None, :]
    shear = young_e[None, None, :] / 2.6
    stress = [[shear * (disp[comp_a][comp_b] + disp[comp_b][comp_a]) + (lame * trace_h if comp_a == comp_b else 0.0) for comp_b in range(3)] for comp_a in range(3)]
    energy = 0.5 * sum((stress[comp_a][comp_b] * disp[comp_a][comp_b] for comp_a in range(3) for comp_b in range(3)))
    kinetic = at_points[:, 0] ** 2 + at_points[:, 1] ** 2 + at_points[:, 2] ** 2
    iso_part = 2.0 * energy - eigen[None, :, None] * density_e[None, None, :] * kinetic
    eshelby = [[(iso_part if comp_a == comp_b else 0.0) - 2.0 * (disp[0][comp_a] * stress[0][comp_b] + disp[1][comp_a] * stress[1][comp_b] + disp[2][comp_a] * stress[2][comp_b]) for comp_b in range(3)] for comp_a in range(3)]
    determinant = inv_jac[0, 0] * (inv_jac[1, 1] * inv_jac[2, 2] - inv_jac[1, 2] * inv_jac[2, 1]) - inv_jac[0, 1] * (inv_jac[1, 0] * inv_jac[2, 2] - inv_jac[1, 2] * inv_jac[2, 0]) + inv_jac[0, 2] * (inv_jac[1, 0] * inv_jac[2, 1] - inv_jac[1, 1] * inv_jac[2, 0])
    factor = (quad_weights[:, None] / determinant)[:, None, :]
    proj = [[factor * (eshelby[comp_a][0] * jac[ref_dir][0] + eshelby[comp_a][1] * jac[ref_dir][1] + eshelby[comp_a][2] * jac[ref_dir][2]) for comp_a in range(3)] for ref_dir in range(3)]
    stacked = jnp.stack([jnp.stack(proj[ref_dir], axis=1) for ref_dir in range(3)], axis=0)
    stacked = stacked.reshape(81, 3 * modes_n, elems)
    return jnp.einsum('xb,xze->zbe', gradients, stacked, precision=highest)

def bernstein(cells, params, count):
    offset = jnp.arange(count, dtype=jnp.int32)[:, None] - 3 * cells[None, :]
    param = params[None, :]
    other = 1.0 - param
    return jnp.where(offset == 0, other ** 3, 0.0) + jnp.where(offset == 1, 3.0 * param * other ** 2, 0.0) + jnp.where(offset == 2, 3.0 * param ** 2 * other, 0.0) + jnp.where(offset == 3, param ** 3, 0.0)

def contract(grads, cells, params, ctrl):
    channels, nodes = grads.shape
    width = math.gcd(nodes, 512)
    count = nodes // width

    def step(total, inputs):
        piece, cell_b, param_b = inputs
        along_x = bernstein(cell_b[0], param_b[0], ctrl)
        along_y = bernstein(cell_b[1], param_b[1], ctrl)
        along_z = bernstein(cell_b[2], param_b[2], ctrl)
        left = (piece[:, None, :] * along_x[None, :, :]).reshape(channels * ctrl, width)
        right = (along_y[:, None, :] * along_z[None, :, :]).reshape(ctrl * ctrl, width)
        return (total + lax.dot_general(left, right, (((1,), (1,)), ((), ())), precision=lax.Precision.HIGHEST), None)
    pieces = grads.reshape(channels, count, width).transpose(1, 0, 2)
    cell_blocks = cells.reshape(3, count, width).transpose(1, 0, 2)
    param_blocks = params.reshape(3, count, width).transpose(1, 0, 2)
    total, _ = lax.scan(step, jnp.zeros((channels * ctrl, ctrl * ctrl), grads.dtype), (pieces, cell_blocks, param_blocks))
    return total.reshape(3, channels // 3, ctrl ** 3)

def reference(modes, connect, ghosts, inv_jacobian, young, density, ffd_cell, ffd_param, eigen):
    flat = modes.reshape(N_SLAB, N_SUB, 3 * MODES, NOWN)

    def partial_value(total, index):
        slab_at = (index // N_SUB).astype(jnp.int32)
        sub_at = (index % N_SUB).astype(jnp.int32)
        ghost_list = ghosts[slab_at, sub_at]
        block_id = ghost_list // IFACE
        node_at = ghost_list % IFACE
        owner_slab = ((slab_at + block_id // 3 - 1) % N_SLAB).astype(jnp.int32)
        owner_sub = jnp.clip(sub_at + block_id % 3 - 1, 0, N_SUB - 1).astype(jnp.int32)
        ghost_vals = flat[owner_slab, owner_sub, :, node_at].T
        slot_vals = jnp.concatenate([flat[slab_at, sub_at], ghost_vals], axis=1)
        slot_cells = jnp.concatenate([ffd_cell[slab_at, sub_at], ffd_cell[owner_slab, owner_sub, :, node_at].T], axis=1)
        slot_params = jnp.concatenate([ffd_param[slab_at, sub_at], ffd_param[owner_slab, owner_sub, :, node_at].T], axis=1)
        columns = connect[slab_at, sub_at]
        contrib = element_block(slot_vals[:, columns], inv_jacobian[slab_at, sub_at], young[slab_at, sub_at], density[slab_at, sub_at], eigen)
        slot_grad = jnp.zeros((3 * MODES, SLOTS), slot_vals.dtype).at[:, columns].add(contrib)
        return (total + contract(slot_grad, slot_cells, slot_params, CTRL), None)
    start = jnp.zeros((3, MODES, NCP), modes.dtype)
    total, _ = lax.scan(partial_value, start, jnp.arange(N_SLAB * N_SUB, dtype=jnp.int32))
    return total * (0.5 / jnp.sqrt(eigen))[None, :, None]
```

```python
import math

import jax
import jax.numpy as jnp
from jax import lax
from jax.experimental import pallas as pl
from jax.experimental.pallas import tpu as pltpu
from jax.sharding import PartitionSpec as P

CTRL = 16
LANES = 128
ROWS = 56
GROUP = 8
ROOT = math.sqrt(0.6)
HALF_ROOT = 0.5 * ROOT
GAUSS = (5.0 / 9.0, 8.0 / 9.0, 5.0 / 9.0)


def interp(low, mid, high):
    even = 0.3 * (low + high) + 0.4 * mid
    odd = HALF_ROOT * (high - low)
    return even - odd, mid, even + odd


def slope(low, mid, high):
    odd = 0.5 * (high - low)
    even = ROOT * (low + high - 2.0 * mid)
    return odd - even, odd, odd + even


def interp_t(low, mid, high):
    total = low + high
    even = 0.3 * total
    odd = HALF_ROOT * (high - low)
    return even - odd, 0.4 * total + mid, even + odd


def slope_t(low, mid, high):
    odd = 0.5 * (low + mid + high)
    even = ROOT * (high - low)
    return even - odd, -2.0 * even, even + odd


def along(axis, fn, grid):
    out = [None] * 27
    step = (9, 3, 1)[axis]
    for start in range(27):
        if (start // step) % 3 == 0:
            line = fn(grid[start], grid[start + step], grid[start + 2 * step])
            for pos in range(3):
                out[start + pos * step] = line[pos]
    return out


def split_pair(value):
    high = value.astype(jnp.bfloat16)
    low = (value - high.astype(jnp.float32)).astype(jnp.bfloat16)
    return high, low


def fill_rows(tab, col, width, modes_k, cells, params):
    comps = len(modes_k)
    modes_n = modes_k[0].shape[0]
    for comp, block in enumerate(modes_k):
        tab[pl.ds(comp * modes_n, modes_n), pl.ds(col, width)] = block
    base = comps * modes_n
    tab[pl.ds(base, 8), pl.ds(col, width)] = jnp.concatenate(
        [cells.astype(jnp.float32), params, jnp.zeros((2, width), jnp.float32)], axis=0
    )


def pack_kernel(modes, cells, params, out):
    width = out.shape[1]
    fill_rows(
        out,
        0,
        width,
        [modes[0, 0, comp, :, :width] for comp in range(3)],
        cells[0, 0, :, :width],
        params[0, 0, :, :width],
    )


def one_hot(index_row, depth, iota):
    width = index_row.shape[1]
    wide = jnp.broadcast_to(index_row, (16, width))
    upper = wide >> 8
    lower = (wide & 255).astype(jnp.float32)
    parts = []
    for chunk in range(depth // 256):
        code = jnp.where(upper == chunk, lower, -1.0).astype(jnp.bfloat16)
        hit = iota.reshape(16, 16, width) == code[None]
        parts.append(
            jnp.where(hit, jnp.bfloat16(1), jnp.bfloat16(0)).reshape(256, width)
        )
    return jnp.concatenate(parts, axis=0)


def bernstein(cell, param, count):
    offset = lax.broadcasted_iota(jnp.int32, (count, LANES), 0) - jnp.broadcast_to(
        3 * cell.astype(jnp.int32), (count, LANES)
    )
    other = 1.0 - param
    square = param * param
    other_square = other * other
    result = jnp.zeros((count, LANES), jnp.float32)
    for which, poly in enumerate(
        (other_square * other, 3.0 * param * other_square, 3.0 * square * other, square * param)
    ):
        result = jnp.where(offset == which, jnp.broadcast_to(poly, (count, LANES)), result)
    return result


def make_kernel(elem_start, nblocks, iface, first):
    def kernel(*refs):
        modes, cells, params, conn, jac, young, density, eigen = refs[:8]
        pos = 8
        if not first:
            ghosts, blocks, acc_in = refs[pos], refs[pos + 1 : pos + 1 + len(nblocks)], refs[
                pos + 1 + len(nblocks)
            ]
            pos += 2 + len(nblocks)
        out = refs[pos]
        tab32, tab, conn_s, iota, vals, field, proj, jac_s, grads = refs[pos + 1 : pos + 10]
        if not first:
            ghost32, ghost_tab = refs[pos + 10 : pos + 12]
        modes_n = modes.shape[3]
        nown = modes.shape[4]
        nodes = conn.shape[2]
        groups = modes_n // GROUP
        lanes = pl.ds(elem_start, LANES)
        fill_rows(
            tab32, 0, nown, [modes[0, 0, comp] for comp in range(3)], cells[0, 0], params[0, 0]
        )
        high, low = split_pair(tab32[...])
        tab[:, pl.ds(0, nown)] = jnp.concatenate([high, low], axis=0)
        iota[...] = lax.broadcasted_iota(jnp.int32, (256, 256), 0).astype(jnp.float32).astype(
            jnp.bfloat16
        )
        depth = nown
        if not first:
            col = 0
            for block, names in zip(blocks, nblocks):
                for name in names:
                    piece = block[...] if name is None else block[name]
                    high, low = split_pair(piece)
                    ghost_tab[:, pl.ds(col, iface)] = jnp.concatenate([high, low], axis=0)
                    col += iface
            nghost = ghosts.shape[2]
            for start in range(0, nghost, 256):
                index = ghosts[0, :, pl.ds(start, 256)]
                picked = jnp.dot(
                    ghost_tab[...],
                    one_hot(index, col, iota[...]),
                    preferred_element_type=jnp.float32,
                )
                tab[:, pl.ds(nown + start, 256)] = picked.astype(jnp.bfloat16)
            depth = nown + nghost
        conn_s[...] = jnp.full(conn_s.shape, -1, jnp.int32)
        conn_s[pl.ds(0, nodes), :] = conn[0, 0, :, lanes]

        def gather(step, carry):
            for inner in range(2):
                node = step * 4 + inner * 2
                index = jnp.concatenate(
                    [conn_s[pl.ds(node, 1), :], conn_s[pl.ds(node + 1, 1), :]], axis=1
                )
                picked = jnp.dot(
                    tab[...],
                    one_hot(index, depth, iota[...]),
                    preferred_element_type=jnp.float32,
                )
                both = picked[:ROWS] + picked[ROWS:]
                vals[node] = both[:, :LANES]
                vals[node + 1] = both[:, LANES:]
            return carry

        lax.fori_loop(0, conn_s.shape[0] // 4, gather, 0)

        inv = [[jac[0, 0, ref_dir, comp, :, lanes] for comp in range(3)] for ref_dir in range(3)]
        det = (
            inv[0][0] * (inv[1][1] * inv[2][2] - inv[1][2] * inv[2][1])
            - inv[0][1] * (inv[1][0] * inv[2][2] - inv[1][2] * inv[2][0])
            + inv[0][2] * (inv[1][0] * inv[2][1] - inv[1][1] * inv[2][0])
        )
        point = lax.broadcasted_iota(jnp.int32, det.shape, 0)
        weight = jnp.ones(det.shape, jnp.float32)
        for digit in (9, 3, 1):
            weight = weight * jnp.where((point // digit) % 3 == 1, GAUSS[1], GAUSS[0])
        factor = 2.0 * weight / det
        for ref_dir in range(3):
            for comp in range(3):
                jac_s[ref_dir * 3 + comp] = inv[ref_dir][comp]
                jac_s[9 + ref_dir * 3 + comp] = inv[ref_dir][comp] * factor
        stiff = young[0, :, lanes]
        lame = jnp.broadcast_to(0.3 / 0.52 * stiff, (GROUP, LANES))
        shear = jnp.broadcast_to(stiff / 2.6, (GROUP, LANES))
        dens = jnp.broadcast_to(density[0, :, lanes], (GROUP, LANES))

        def element(group, carry):
            modes_at = pl.multiple_of(group * GROUP, GROUP)
            eig = jnp.broadcast_to(eigen[pl.ds(modes_at, GROUP), :], (GROUP, LANES))
            inertia = eig * dens
            scale = 0.5 / jnp.sqrt(eig)
            for comp in range(3):
                grid = [
                    vals[node, pl.ds(comp * modes_n + modes_at, GROUP), :] for node in range(27)
                ]
                x_in = along(0, interp, grid)
                x_sl = along(0, slope, grid)
                xy_in = along(1, interp, x_in)
                for which, res in (
                    (0, along(2, interp, along(1, interp, x_sl))),
                    (1, along(2, interp, along(1, slope, x_in))),
                    (2, along(2, slope, xy_in)),
                    (3, along(2, interp, xy_in)),
                ):
                    for q in range(27):
                        field[which, q, comp] = res[q]

            def at_point(q, inner_carry):
                ref = [[field[which, q, comp] for comp in range(3)] for which in range(4)]
                jm = [
                    [
                        jnp.broadcast_to(jac_s[d * 3 + j, pl.ds(q, 1), :], (GROUP, LANES))
                        for j in range(3)
                    ]
                    for d in range(3)
                ]
                js = [
                    [
                        jnp.broadcast_to(jac_s[9 + d * 3 + j, pl.ds(q, 1), :], (GROUP, LANES))
                        for j in range(3)
                    ]
                    for d in range(3)
                ]
                disp = [
                    [
                        ref[0][k] * jm[0][j] + ref[1][k] * jm[1][j] + ref[2][k] * jm[2][j]
                        for j in range(3)
                    ]
                    for k in range(3)
                ]
                trace = lame * (disp[0][0] + disp[1][1] + disp[2][2])
                twice = shear + shear
                diag = [twice * disp[k][k] + trace for k in range(3)]
                sums = {
                    (0, 1): disp[0][1] + disp[1][0],
                    (0, 2): disp[0][2] + disp[2][0],
                    (1, 2): disp[1][2] + disp[2][1],
                }
                off = {pair: shear * value for pair, value in sums.items()}

                def sigma(k, j):
                    return diag[k] if k == j else off[(min(k, j), max(k, j))]

                work = (
                    diag[0] * disp[0][0]
                    + diag[1] * disp[1][1]
                    + diag[2] * disp[2][2]
                    + off[(0, 1)] * sums[(0, 1)]
                    + off[(0, 2)] * sums[(0, 2)]
                    + off[(1, 2)] * sums[(1, 2)]
                )
                kinetic = ref[3][0] * ref[3][0] + ref[3][1] * ref[3][1] + ref[3][2] * ref[3][2]
                iso = 0.5 * (work - inertia * kinetic)
                for d in range(3):
                    tau = [
                        js[d][0] * sigma(k, 0) + js[d][1] * sigma(k, 1) + js[d][2] * sigma(k, 2)
                        for k in range(3)
                    ]
                    for i in range(3):
                        proj[d, q, i] = iso * js[d][i] - (
                            disp[0][i] * tau[0] + disp[1][i] * tau[1] + disp[2][i] * tau[2]
                        )
                return inner_carry

            lax.fori_loop(0, 27, at_point, 0)
            for comp in range(3):
                px = along(1, interp_t, along(2, interp_t, [proj[0, q, comp] for q in range(27)]))
                py = along(1, slope_t, along(2, interp_t, [proj[1, q, comp] for q in range(27)]))
                pz = along(1, interp_t, along(2, slope_t, [proj[2, q, comp] for q in range(27)]))
                from_x = along(0, slope_t, px)
                from_yz = along(0, interp_t, [first_v + second_v for first_v, second_v in zip(py, pz)])
                for node in range(27):
                    grads[
                        node, pl.ds(group * (3 * GROUP) + comp * GROUP, GROUP), :
                    ] = scale * (from_x[node] + from_yz[node])
            return carry

        lax.fori_loop(0, groups, element, 0)
        grads[27] = jnp.zeros((3 * modes_n, LANES), jnp.float32)
        base = 3 * modes_n
        if first:
            out[...] = jnp.zeros(out.shape, jnp.float32)
        else:
            out[...] = acc_in[...]

        def contract(step, carry):
            lefts = []
            rights = []
            for inner in range(2):
                node = step * 2 + inner
                rows = vals[node, pl.ds(base, 8), :]
                along_x, along_y, along_z = [
                    bernstein(rows[dim : dim + 1], rows[3 + dim : 4 + dim], CTRL)
                    for dim in range(3)
                ]
                piece = grads[node]
                left = (along_x[:, None, :] * piece[None, :, :]).reshape(
                    CTRL * 3 * modes_n, LANES
                )
                right = (along_y[:, None, :] * along_z[None, :, :]).reshape(CTRL * CTRL, LANES)
                lefts.append(split_pair(left))
                rights.append(split_pair(right))
            left_all = jnp.concatenate(
                [lefts[0][0], lefts[1][0], lefts[0][0], lefts[1][0], lefts[0][1], lefts[1][1]],
                axis=1,
            )
            right_all = jnp.concatenate(
                [
                    rights[0][0],
                    rights[1][0],
                    rights[0][1],
                    rights[1][1],
                    rights[0][0],
                    rights[1][0],
                ],
                axis=1,
            )
            out[...] += lax.dot_general(
                left_all,
                right_all,
                (((1,), (1,)), ((), ())),
                preferred_element_type=jnp.float32,
            )
            return carry

        lax.fori_loop(0, 14, contract, 0)

    return kernel


def run_elements(elem_start, arrays, halo, acc):
    modes, connect, jac = arrays[0], arrays[3], arrays[4]
    modes_n, nown = modes.shape[3], modes.shape[4]
    channels = 3 * modes_n
    operands = list(arrays)
    nblocks = ()
    iface = 0
    nghost = 0
    extra = []
    if halo is not None:
        ghosts, blocks, nblocks = halo
        iface = blocks[0].shape[-1]
        nghost = ghosts.shape[2]
        operands += [ghosts, *blocks, acc]
        total = sum(len(names) for names in nblocks)
        extra = [
            pltpu.VMEM((8, LANES), jnp.float32),
            pltpu.VMEM((2 * ROWS, total * iface), jnp.bfloat16),
        ]
    f32 = jnp.float32
    scratch = [
        pltpu.VMEM((ROWS, nown), f32),
        pltpu.VMEM((2 * ROWS, nown + nghost), jnp.bfloat16),
        pltpu.VMEM((28, LANES), jnp.int32),
        pltpu.VMEM((256, 256), jnp.bfloat16),
        pltpu.VMEM((28, ROWS, LANES), f32),
        pltpu.VMEM((4, 27, 3, GROUP, LANES), f32),
        pltpu.VMEM((3, 27, 3, GROUP, LANES), f32),
        pltpu.VMEM((18, 27, LANES), f32),
        pltpu.VMEM((28, channels, LANES), f32),
    ] + extra
    return pl.pallas_call(
        make_kernel(elem_start, nblocks, iface, halo is None),
        out_shape=jax.ShapeDtypeStruct((CTRL * channels, CTRL * CTRL), f32),
        scratch_shapes=scratch,
        cost_estimate=pl.CostEstimate(
            flops=4_000_000_000, transcendentals=0, bytes_accessed=4_000_000
        ),
        name="inner_elements" if halo is None else "outer_elements",
    )(*operands)


def exchange(block, axis, forward):
    return lax.ppermute(block, axis, forward)


def on_device(modes, connect, ghosts, inv_jacobian, young, density, ffd_cell, ffd_param, eigen):
    modes_n, nown = modes.shape[3], modes.shape[4]
    elems = connect.shape[3]
    iface = nown // 4
    n_slab, n_sub = lax.axis_size("slab"), lax.axis_size("sub")
    payload = pl.pallas_call(
        pack_kernel,
        out_shape=jax.ShapeDtypeStruct((ROWS, iface), jnp.float32),
        name="pack",
    )(modes, ffd_cell, ffd_param)
    ring = [(i, (i + 1) % n_slab) for i in range(n_slab)]
    back = [(target, source) for source, target in ring]
    block_id = ghosts // iface
    node_at = ghosts % iface
    if n_sub == 2:
        other = lax.ppermute(payload, "sub", [(0, 1), (1, 0)])
        both = jnp.stack([payload, other])
        below = lax.ppermute(both, "slab", ring)
        above = lax.ppermute(both, "slab", back)
        part_a = block_id // 3
        beside = (block_id % 3 != 1).astype(jnp.int32)
        place = jnp.where(part_a == 0, beside, jnp.where(part_a == 1, 2, 3 + beside))
        blocks, names = [below, other, above], ((0, 1), (None,), (0, 1))
    else:
        up = [(i, i + 1) for i in range(n_sub - 1)]
        down = [(target, source) for source, target in up]
        three = jnp.stack(
            [
                lax.ppermute(payload, "sub", up),
                payload,
                lax.ppermute(payload, "sub", down),
            ]
        )
        below = lax.ppermute(three, "slab", ring)
        above = lax.ppermute(three, "slab", back)
        place = block_id
        blocks, names = [below, three, above], ((0, 1, 2),) * 3
    arrays = (
        modes,
        ffd_cell,
        ffd_param,
        connect,
        inv_jacobian,
        young,
        density,
        eigen.reshape(modes_n, 1),
    )
    acc = run_elements(0, arrays, None, None)
    total = run_elements(
        elems // 2, arrays, (place * iface + node_at, blocks, names), acc
    )
    plane = CTRL * CTRL
    if n_slab == CTRL and n_sub == modes_n // GROUP == 2:
        block = total.reshape(CTRL, n_sub, 3 * GROUP, plane)
        return reduce_scatter(block, n_slab).reshape(3, GROUP, plane)
    groups = modes_n // GROUP
    design = (
        total.reshape(CTRL, groups, 3, GROUP, plane)
        .transpose(2, 1, 3, 0, 4)
        .reshape(3, modes_n, CTRL * plane)
    )
    by_cycle = lax.psum_scatter(design, "slab", scatter_dimension=2, tiled=True)
    return lax.psum_scatter(by_cycle, "sub", scatter_dimension=1, tiled=True)


def halve(block, dim, bit, axis, pairs):
    keep = lax.dynamic_index_in_dim(block, bit, dim, keepdims=False)
    send = lax.dynamic_index_in_dim(block, 1 - bit, dim, keepdims=False)
    return keep + lax.ppermute(send, axis, pairs)


def reduce_scatter(block, n_slab):
    place = lax.axis_index("slab")
    bits = n_slab.bit_length() - 1
    block = block.reshape((2,) * bits + block.shape[1:])

    def by_slab(value, power, dim):
        pairs = [(i, i ^ power) for i in range(n_slab)]
        return halve(value, dim, (place // power) % 2, "slab", pairs)

    block = by_slab(block, 1, bits - 1)
    block = halve(block, bits - 1, lax.axis_index("sub"), "sub", [(0, 1), (1, 0)])
    for level in range(1, bits):
        block = by_slab(block, 1 << level, bits - 1 - level)
    return block


def solution(mesh):
    return jax.shard_map(
        on_device,
        mesh=mesh,
        in_specs=(
            P("slab", "sub", None, None, None),
            P("slab", "sub", None, None),
            P("slab", "sub", None),
            P("slab", "sub", None, None, None, None),
            P("slab", "sub", None),
            P("slab", "sub", None),
            P("slab", "sub", None, None),
            P("slab", "sub", None, None),
            P(),
        ),
        out_specs=P(None, "sub", "slab"),
        check_vma=False,
    )
```
